32 devices in a mesh: row: 4 (over y, x), col: 8 (over z, core).
Axes of the slice: x: 2, y: 2, z: 4, core: 2. Of those that a mesh axis runs over, the one named last changes fastest.
Arguments:
- pair_rep: bfloat16 [256, 256, 128], P('row', 'col'), may hold values from -6 to 6
- proj_weight: bfloat16 [2, 4, 128, 128], replicated, may hold values from -0.5 to 0.5
- gate_weight: bfloat16 [2, 128, 128], replicated, may hold values from -0.5 to 0.5
- out_weight: bfloat16 [2, 128, 128], replicated, may hold values from -0.5 to 0.5
- in_gain: float32 [2, 128], replicated, may hold values from 0.1 to 1.9
- out_gain: float32 [2, 128], replicated, may hold values from 0.1 to 1.9
Outputs:
- updated_pair: bfloat16 [256, 256, 128], P('row', 'col')
The draws below stay inside these ranges and needn't reach their ends.
All inputs are finite; a program needn't handle non-finite values.
Results may differ from the reference program's by a relative error of at most 0.011.
Values may be sent and summed in bfloat16 or wider, within the bound.
A program may use at most 64 MiB of HBM per device.

```python
import math
import jax
import jax.numpy as jnp
from jax import lax

C = 128
H = 128
N = 256


def steps_of(own_key, extent, cuts, smallest, largest):
    def one(position, parts):
        draws = jax.random.uniform(jax.random.fold_in(jax.random.fold_in(own_key, 6), position), (parts,), jnp.float32, smallest / len(cuts), largest / len(cuts))
        return jnp.repeat(jnp.exp(draws), extent[position] // parts).reshape((-1,) + (1,) * (len(extent) - position - 1))

    level = one(*cuts[0])
    for cut in cuts[1:]:
        level = level * one(*cut)
    return level


def noise(key, extent, deviation, most, cuts=(), kind=jnp.bfloat16):
    entries = jax.random.normal(key, extent, jnp.float32) * deviation
    if len(cuts) > 0:
        entries = steps_of(key, extent, cuts, -0.22, 0.18) * entries
    return jnp.clip(entries, min=-most, max=most).astype(kind)


def setup_inputs(seed: int = 0) -> dict:
    arg_keys = jax.random.split(jax.random.key(seed), 7)
    pair_rep = noise(arg_keys[0], (N, N, C), 1.0, 6.0, ((0, 4), (1, 8)))
    proj_weight = noise(arg_keys[1], (2, 4, C, H), C ** -0.5, 0.5)
    gate_weight = noise(arg_keys[2], (2, C, C), C ** -0.5, 0.5)
    out_weight = noise(arg_keys[3], (2, H, C), H ** -0.5, 0.5)
    in_gain = jnp.clip(1.0 + 0.18 * jax.random.normal(arg_keys[4], (2, C), jnp.float32), 0.1, 1.9)
    out_gain = jnp.clip(1.0 + 0.18 * jax.random.normal(arg_keys[5], (2, H), jnp.float32), 0.1, 1.9)
    return dict(pair_rep=pair_rep, proj_weight=proj_weight, gate_weight=gate_weight, out_weight=out_weight, in_gain=in_gain, out_gain=out_gain)


epsilon = 1e-05

def layer_norm(values, gain_row):
    center = values - lax.optimization_barrier(jnp.mean(values, axis=-1, keepdims=True))
    spread = lax.optimization_barrier(jnp.mean(center * center, axis=-1, keepdims=True))
    return center * lax.rsqrt(spread + epsilon) * gain_row

def reference(pair_rep, proj_weight, gate_weight, out_weight, in_gain, out_gain):
    row_block = math.gcd(N, 64)
    channel_block = math.gcd(H, 16)
    current = pair_rep
    for update_index in range(2):
        weight_joined = jnp.transpose(proj_weight[update_index], (1, 0, 2)).reshape(C, 4 * H)

        def project(row_slab):
            widened = row_slab.astype(jnp.float32)
            normed = layer_norm(widened, in_gain[update_index]).astype(jnp.bfloat16)
            projected = jnp.dot(normed, weight_joined, preferred_element_type=jnp.float32)
            left_hand = (jax.nn.sigmoid(projected[..., 0:H]) * projected[..., H:2 * H]).astype(jnp.bfloat16)
            right_hand = (jax.nn.sigmoid(projected[..., 2 * H:3 * H]) * projected[..., 3 * H:4 * H]).astype(jnp.bfloat16)
            gating = jax.nn.sigmoid(jnp.dot(normed, gate_weight[update_index], preferred_element_type=jnp.float32))
            return (left_hand, right_hand, gating)
        blocks = current.reshape(N // row_block, row_block, N, C)
        left_hand, right_hand, gating = lax.map(project, blocks)
        left_channels = jnp.moveaxis(left_hand.reshape(N, N, H), 2, 0).reshape(H // channel_block, channel_block, N, N)
        right_channels = jnp.moveaxis(right_hand.reshape(N, N, H), 2, 0).reshape(H // channel_block, channel_block, N, N)
        pattern = 'hik,hjk->hij' if update_index == 0 else 'hki,hkj->hij'

        def contract(operands):
            return jnp.einsum(pattern, operands[0].astype(jnp.float32), operands[1].astype(jnp.float32)).astype(jnp.bfloat16)
        triangle = lax.map(contract, (left_channels, right_channels))
        triangle = jnp.moveaxis(triangle.reshape(H, N, N), 0, 2)

        def finish(pieces):
            triangle_rows, gate_rows, old_rows = pieces
            mixed = layer_norm(triangle_rows.astype(jnp.float32), out_gain[update_index]).astype(jnp.bfloat16)
            update = jnp.dot(mixed, out_weight[update_index], preferred_element_type=jnp.float32)
            return (old_rows.astype(jnp.float32) + gate_rows * update).astype(jnp.bfloat16)
        current = lax.map(finish, (triangle.reshape(N // row_block, row_block, N, H), gating, blocks)).reshape(N, N, C)
    return current
```

```python
import functools

import jax
import jax.numpy as jnp
from jax import lax
from jax.experimental import pallas as pl
from jax.experimental.pallas import tpu as pltpu
from jax.sharding import PartitionSpec as P

epsilon = 1e-05
LANES = 128
PACK = 16
f32 = jnp.float32
bf16 = jnp.bfloat16


def layer_norm(values, gain_row, reduce_axis):
    center = values - jnp.mean(values, axis=reduce_axis, keepdims=True)
    spread = jnp.mean(center * center, axis=reduce_axis, keepdims=True)
    return center * lax.rsqrt(spread + epsilon) * gain_row


def plain(pair_rep, proj_weight, gate_weight, out_weight, in_gain, out_gain):
    current = pair_rep
    for update_index in range(2):
        widened = current.astype(f32)
        normed = layer_norm(widened, in_gain[update_index], 2).astype(bf16)
        projected = jnp.einsum(
            "ijc,pch->phij", normed, proj_weight[update_index], preferred_element_type=f32
        )
        left_hand = (jax.nn.sigmoid(projected[0]) * projected[1]).astype(bf16)
        right_hand = (jax.nn.sigmoid(projected[2]) * projected[3]).astype(bf16)
        gating = jax.nn.sigmoid(
            jnp.dot(normed, gate_weight[update_index], preferred_element_type=f32)
        )
        left_rows, right_rows = (
            lax.all_to_all(left_hand, "col", split_axis=0, concat_axis=2, tiled=True),
            lax.all_to_all(right_hand, "col", split_axis=0, concat_axis=2, tiled=True),
        )
        if update_index == 0:
            triangle = jnp.einsum(
                "gik,gjk->igj",
                left_rows,
                lax.all_gather(right_rows, "row", axis=1, tiled=True),
                preferred_element_type=f32,
            )
        else:
            left_columns = lax.all_to_all(left_rows, "row", split_axis=2, concat_axis=1, tiled=True)
            triangle = jnp.einsum(
                "gki,gkj->igj",
                left_columns,
                lax.all_gather(right_rows, "row", axis=1, tiled=True),
                preferred_element_type=f32,
            )
        returned = lax.all_to_all(
            triangle.astype(bf16), "col", split_axis=2, concat_axis=1, tiled=True
        )
        mixed_rows = layer_norm(
            returned.astype(f32), out_gain[update_index][None, :, None], 1
        ).astype(bf16)
        update = jnp.einsum(
            "ihj,hc->ijc", mixed_rows, out_weight[update_index], preferred_element_type=f32
        )
        current = (widened + gating * update).astype(bf16)
    return current


def norm_columns(values, gain_column):
    scale = 1.0 / values.shape[0]
    center = values - jnp.sum(values, axis=0, keepdims=True) * scale
    spread = jnp.sum(center * center, axis=0, keepdims=True) * scale
    return center * lax.rsqrt(spread + epsilon) * gain_column


def kernel(rows, cols, x_ref, pw_ref, gw_ref, ow_ref, ig_ref, og_ref, o_ref,
           xt, nt, gt, tt, wt, gwt, owt, perm, shuffle, back,
           send_lr, recv_lr, send_t, recv_t, ml, mr,
           ss_lr, rs_lr, ss_t, rs_t):
    devices = rows * cols
    first, second, channels = x_ref.shape
    hidden = ow_ref.shape[1]
    fold = LANES // second
    depth = first // fold
    chunks = hidden // devices
    groups = cols // fold
    width = depth * LANES
    step = min(width, 512)
    my_row, my_col = lax.axis_index("row"), lax.axis_index("col")
    me = my_row * cols + my_col

    def partner(n):
        m = lax.rem(n * 13, devices) if devices % 13 else n
        return lax.rem(my_row + m % rows, rows), lax.rem(my_col + m // rows, cols)

    barrier = pltpu.get_barrier_semaphore()

    @pl.loop(1, devices)
    def _(n):
        pl.semaphore_signal(barrier, inc=1, device_id=partner(n), device_id_type=pl.DeviceIdType.MESH)

    for u in range(2):
        for p in range(4):
            turned = pw_ref[u, p].astype(f32).T.astype(bf16)
            for c in range(chunks):
                wt[u, c, p * devices:(p + 1) * devices, :] = turned[c * devices:(c + 1) * devices]
        gwt[u] = gw_ref[u].astype(f32).T.astype(bf16)
        owt[u] = ow_ref[u].astype(f32).T.astype(bf16)
    size = fold * LANES
    to = lax.broadcasted_iota(jnp.int32, (size, size), 1)
    at = lax.broadcasted_iota(jnp.int32, (size, size), 0)
    wanted = (to % LANES) // second * LANES + to // LANES * second + to % second
    perm[...] = jnp.where(at == wanted, 1.0, 0.0).astype(bf16)
    for q in range(depth):
        tile = jnp.concatenate([x_ref[a * depth + q] for a in range(fold)], axis=0)
        xt[:, q * LANES:(q + 1) * LANES] = tile.astype(f32).T

    def start(send, recv, ssem, rsem, slot):
        pltpu.make_async_copy(send.at[slot, me], recv.at[slot, me], rsem.at[slot]).start()

        @pl.loop(1, devices)
        def _(n):
            row, col = partner(n)
            pltpu.make_async_remote_copy(
                src_ref=send.at[slot, row * cols + col],
                dst_ref=recv.at[slot, me],
                send_sem=ssem.at[slot],
                recv_sem=rsem.at[slot],
                device_id=(row, col),
                device_id_type=pl.DeviceIdType.MESH,
            ).start()

    for u in range(2):
        gain_in = jnp.broadcast_to(ig_ref[u:u + 1, :], (LANES, channels)).T[:, :1]
        gain_out = jnp.broadcast_to(og_ref[u:u + 1, :], (LANES, hidden)).T[:, :1]
        for t in range(0, width, step):
            nt[:, t:t + step] = norm_columns(xt[:, t:t + step], gain_in).astype(bf16)
        for c in range(chunks):
            slot = u * chunks + c
            for t in range(0, width, step):
                got = jnp.dot(wt[u, c], nt[:, t:t + step], preferred_element_type=f32)
                for s in range(2):
                    base = 2 * s * devices
                    hand = jax.nn.sigmoid(got[base:base + devices]) * got[base + devices:base + 2 * devices]
                    for k in range(step // LANES):
                        shuffle[s, pl.ds(t // LANES + k, devices, stride=depth), :] = (
                            hand[:, k * LANES:(k + 1) * LANES]
                        )
            for s in range(2):
                send_lr[slot, :, s] = shuffle[s].reshape(devices, depth, LANES).astype(bf16)
            if slot == 0:
                pl.semaphore_wait(barrier, devices - 1)
            start(send_lr, recv_lr, ss_lr, rs_lr, slot)
        for t in range(0, width, step):
            gt[:, t:t + step] = jax.nn.sigmoid(
                jnp.dot(gwt[u], nt[:, t:t + step], preferred_element_type=f32)
            )
        for c in range(chunks):
            slot = u * chunks + c
            pltpu.make_async_copy(recv_lr.at[slot], recv_lr.at[slot], rs_lr.at[slot]).wait()
            for s, matrix in enumerate((ml, mr)):
                wide = jnp.concatenate([
                    jnp.concatenate([
                        recv_lr[slot, r * cols + g * fold + e, s]
                        for r in range(rows) for g in range(groups)
                    ], axis=0)
                    for e in range(fold)
                ], axis=1)
                moved = jnp.dot(wide, perm[...], preferred_element_type=f32).astype(bf16)
                for r in range(rows):
                    for g in range(groups):
                        for a in range(fold):
                            matrix[r * first + a * depth:r * first + (a + 1) * depth,
                                   g * LANES:(g + 1) * LANES] = (
                                moved[(r * groups + g) * depth:(r * groups + g + 1) * depth,
                                      a * LANES:(a + 1) * LANES]
                            )
            axis = 1 if u == 0 else 0
            tri = lax.dot_general(
                ml[...], mr[...], (((axis,), (axis,)), ((), ())), preferred_element_type=f32
            ).astype(bf16)
            wide = jnp.concatenate([
                jnp.concatenate([
                    tri[r * first + a * depth:r * first + (a + 1) * depth, g * LANES:(g + 1) * LANES]
                    for r in range(rows) for g in range(groups)
                ], axis=0)
                for a in range(fold)
            ], axis=1)
            moved = jnp.dot(wide, perm[...], preferred_element_type=f32).astype(bf16)
            for r in range(rows):
                for g in range(groups):
                    for e in range(fold):
                        send_t[slot, r * cols + g * fold + e] = (
                            moved[(r * groups + g) * depth:(r * groups + g + 1) * depth,
                                  e * LANES:(e + 1) * LANES]
                        )
            start(send_t, recv_t, ss_t, rs_t, slot)
        for c in range(chunks):
            slot = u * chunks + c
            pltpu.make_async_copy(recv_t.at[slot], recv_t.at[slot], rs_t.at[slot]).wait()
            back[...] = recv_t[slot].astype(f32).reshape(devices * depth, LANES)
            for q in range(depth):
                tt[c * devices:(c + 1) * devices, q * LANES:(q + 1) * LANES] = (
                    back[pl.ds(q, devices, stride=depth), :]
                )
        for t in range(0, width, step):
            mixed = norm_columns(tt[:, t:t + step], gain_out).astype(bf16)
            update = jnp.dot(owt[u], mixed, preferred_element_type=f32)
            xt[:, t:t + step] = (
                (xt[:, t:t + step] + gt[:, t:t + step] * update).astype(bf16).astype(f32)
            )
    for q in range(depth):
        tile = xt[:, q * LANES:(q + 1) * LANES].T.astype(bf16)
        for a in range(fold):
            o_ref[a * depth + q] = tile[a * second:(a + 1) * second]
    for slot in range(2 * chunks):
        for send, ssem in ((send_lr, ss_lr), (send_t, ss_t)):
            sent = send.at[slot, pl.ds(0, devices - 1)]
            pltpu.make_async_copy(sent, sent, ssem.at[slot]).wait()


def takes(rows, cols, first, second, channels, hidden):
    devices = rows * cols
    if LANES % second or second > LANES or channels != LANES or hidden % devices or devices % PACK:
        return False
    fold = LANES // second
    return (
        first % fold == 0 and (first // fold) % PACK == 0 and cols % fold == 0
        and hidden * first * second * 4 <= 2 ** 21
    )


def solution(mesh):
    rows, cols = mesh.shape["row"], mesh.shape["col"]

    def local(pair_rep, proj_weight, gate_weight, out_weight, in_gain, out_gain):
        first, second, channels = pair_rep.shape
        hidden = out_weight.shape[1]
        args = (pair_rep, proj_weight, gate_weight, out_weight, in_gain, out_gain)
        if not takes(rows, cols, first, second, channels, hidden):
            return plain(*args)
        devices = rows * cols
        fold = LANES // second
        depth = first // fold
        chunks = hidden // devices
        width = depth * LANES
        vmem = pl.BlockSpec(memory_space=pltpu.VMEM)
        return pl.pallas_call(
            functools.partial(kernel, rows, cols),
            out_shape=jax.ShapeDtypeStruct(pair_rep.shape, bf16),
            in_specs=[vmem] * 6,
            out_specs=vmem,
            scratch_shapes=[
                pltpu.VMEM((channels, width), f32),
                pltpu.VMEM((channels, width), bf16),
                pltpu.VMEM((channels, width), f32),
                pltpu.VMEM((hidden, width), f32),
                pltpu.VMEM((2, chunks, 4 * devices, channels), bf16),
                pltpu.VMEM((2, channels, channels), bf16),
                pltpu.VMEM((2, channels, hidden), bf16),
                pltpu.VMEM((fold * LANES, fold * LANES), bf16),
                pltpu.VMEM((2, devices * depth, LANES), f32),
                pltpu.VMEM((devices * depth, LANES), f32),
                pltpu.VMEM((2 * chunks, devices, 2, depth, LANES), bf16),
                pltpu.VMEM((2 * chunks, devices, 2, depth, LANES), bf16),
                pltpu.VMEM((2 * chunks, devices, depth, LANES), bf16),
                pltpu.VMEM((2 * chunks, devices, depth, LANES), bf16),
                pltpu.VMEM((rows * first, cols * second), bf16),
                pltpu.VMEM((rows * first, cols * second), bf16),
                pltpu.SemaphoreType.DMA((2 * chunks,)),
                pltpu.SemaphoreType.DMA((2 * chunks,)),
                pltpu.SemaphoreType.DMA((2 * chunks,)),
                pltpu.SemaphoreType.DMA((2 * chunks,)),
            ],
            compiler_params=pltpu.CompilerParams(collective_id=0, has_side_effects=True),
        )(*args)

    return jax.shard_map(
        local,
        mesh=mesh,
        in_specs=(P("row", "col", None), P(), P(), P(), P(), P()),
        out_specs=P("row", "col", None),
        check_vma=False,
    )
```

```python
import functools

import jax
import jax.numpy as jnp
from jax import lax
from jax.experimental import pallas as pl
from jax.experimental.pallas import tpu as pltpu
from jax.sharding import PartitionSpec as P

epsilon = 1e-05
LANES = 128
PACK = 16
CHUNK = 32
f32 = jnp.float32
bf16 = jnp.bfloat16


def layer_norm(values, gain_row, reduce_axis):
    center = values - jnp.mean(values, axis=reduce_axis, keepdims=True)
    spread = jnp.mean(center * center, axis=reduce_axis, keepdims=True)
    return center * lax.rsqrt(spread + epsilon) * gain_row


def plain(pair_rep, proj_weight, gate_weight, out_weight, in_gain, out_gain):
    current = pair_rep
    for update_index in range(2):
        widened = current.astype(f32)
        normed = layer_norm(widened, in_gain[update_index], 2).astype(bf16)
        projected = jnp.einsum(
            "ijc,pch->phij", normed, proj_weight[update_index], preferred_element_type=f32
        )
        left_hand = (jax.nn.sigmoid(projected[0]) * projected[1]).astype(bf16)
        right_hand = (jax.nn.sigmoid(projected[2]) * projected[3]).astype(bf16)
        gating = jax.nn.sigmoid(
            jnp.dot(normed, gate_weight[update_index], preferred_element_type=f32)
        )
        left_rows, right_rows = (
            lax.all_to_all(left_hand, "col", split_axis=0, concat_axis=2, tiled=True),
            lax.all_to_all(right_hand, "col", split_axis=0, concat_axis=2, tiled=True),
        )
        if update_index == 0:
            triangle = jnp.einsum(
                "gik,gjk->igj",
                left_rows,
                lax.all_gather(right_rows, "row", axis=1, tiled=True),
                preferred_element_type=f32,
            )
        else:
            left_columns = lax.all_to_all(left_rows, "row", split_axis=2, concat_axis=1, tiled=True)
            triangle = jnp.einsum(
                "gki,gkj->igj",
                left_columns,
                lax.all_gather(right_rows, "row", axis=1, tiled=True),
                preferred_element_type=f32,
            )
        returned = lax.all_to_all(
            triangle.astype(bf16), "col", split_axis=2, concat_axis=1, tiled=True
        )
        mixed_rows = layer_norm(
            returned.astype(f32), out_gain[update_index][None, :, None], 1
        ).astype(bf16)
        update = jnp.einsum(
            "ihj,hc->ijc", mixed_rows, out_weight[update_index], preferred_element_type=f32
        )
        current = (widened + gating * update).astype(bf16)
    return current


def norm_columns(values, gain_column):
    scale = 1.0 / values.shape[0]
    center = values - jnp.sum(values, axis=0, keepdims=True) * scale
    spread = jnp.sum(center * center, axis=0, keepdims=True) * scale
    return center * lax.rsqrt(spread + epsilon) * gain_column


def kernel(rows, cols, x_ref, pw_ref, gw_ref, ow_ref, ig_ref, og_ref, o_ref,
           xt, nt, gt, tt, wt, gwt, owt, perm, shuffle, back,
           send_h, recv_h0, recv_l1, recv_r1, send_t0, recv_t0, send_t1, recv_t1, ml, mr, sems):
    first, second, channels = x_ref.shape
    hidden = ow_ref.shape[1]
    side = cols // 2
    team = rows * side
    fold = LANES // second
    depth = first // fold
    block = CHUNK
    chunks = hidden // block
    each = block // team
    groups = side // fold
    width = depth * LANES
    step = min(width, 512)
    my_row, my_col = lax.axis_index("row"), lax.axis_index("col")
    my_half, my_side = my_col // side, my_col % side
    me = my_row * side + my_side

    def mate(n):
        m = (n * 13) % team if team % 13 else n
        row, place = (my_row + m % rows) % rows, (my_side + m // rows) % side
        return row, place

    def device(n, other):
        row, place = mate(n)
        return row, (1 - my_half if other else my_half) * side + place

    barrier = pltpu.get_barrier_semaphore()

    def greet(n, other):
        pl.semaphore_signal(
            barrier, inc=1, device_id=device(n, other), device_id_type=pl.DeviceIdType.MESH
        )

    greet(0, True)

    @pl.loop(1, team)
    def _(n):
        greet(n, True)
        greet(n, False)

    def send(source, target, kind, slot, n, other):
        row, place = mate(n)
        pltpu.make_async_remote_copy(
            src_ref=source(row, place, other),
            dst_ref=target,
            send_sem=sems.at[2 * kind, slot],
            recv_sem=sems.at[2 * kind + 1, slot],
            device_id=device(n, other),
            device_id_type=pl.DeviceIdType.MESH,
        ).start()

    def keep(source, target, kind, slot):
        pltpu.make_async_copy(
            source(my_row, my_side, False), target, sems.at[2 * kind + 1, slot]
        ).start()

    def arrive(buffer, kind, slot):
        pltpu.make_async_copy(buffer, buffer, sems.at[2 * kind + 1, slot]).wait()

    def weight_turn(u):
        for p in range(4):
            turned = pw_ref[u, p].astype(f32).T.astype(bf16)
            for c in range(chunks):
                wt[u, c, p * block:(p + 1) * block, :] = turned[c * block:(c + 1) * block]

    weight_turn(0)
    for q in range(depth):
        tile = jnp.concatenate([x_ref[a * depth + q] for a in range(fold)], axis=0)
        xt[:, q * LANES:(q + 1) * LANES] = tile.astype(f32).T

    def rest_of_setup():
        weight_turn(1)
        for u in range(2):
            gwt[u] = gw_ref[u].astype(f32).T.astype(bf16)
            owt[u] = ow_ref[u].astype(f32).T.astype(bf16)
        size = fold * LANES
        bits, low = LANES.bit_length() - 1, second.bit_length() - 1
        to = lax.broadcasted_iota(jnp.int32, (1, size), 1)
        at = lax.broadcasted_iota(jnp.int32, (size, size), 0)
        wanted = (
            (((to & (LANES - 1)) >> low) << bits) + ((to >> bits) << low) + (to & (second - 1))
        )
        perm[...] = jnp.where(at == wanted, 1.0, 0.0).astype(bf16)

    def regroup(parts):
        wide = jnp.concatenate([jnp.concatenate(tiles, axis=0) for tiles in parts], axis=1)
        return jnp.dot(wide, perm[...], preferred_element_type=f32).astype(bf16)

    def tile_of(array, row, lane):
        return array[row * depth:(row + 1) * depth, lane * LANES:(lane + 1) * LANES]

    for u in range(2):
        gain_in = jnp.broadcast_to(ig_ref[u:u + 1, :], (LANES, channels)).T[:, :1]
        gain_out = jnp.broadcast_to(og_ref[u:u + 1, :], (LANES, hidden)).T[:, :1]
        for t in range(0, width, step):
            nt[:, t:t + step] = norm_columns(xt[:, t:t + step], gain_in).astype(bf16)
        for c in range(chunks):
            for t in range(0, width, step):
                got = jnp.dot(wt[u, c], nt[:, t:t + step], preferred_element_type=f32)
                for s in range(2):
                    base = 2 * s * block
                    hand = jax.nn.sigmoid(got[base:base + block]) * got[base + block:base + 2 * block]
                    for k in range(step // LANES):
                        shuffle[s, pl.ds(t // LANES + k, block, stride=depth), :] = (
                            hand[:, k * LANES:(k + 1) * LANES]
                        )
            for s in range(2):
                send_h[u, c, :, s] = shuffle[s].reshape(team, each, depth, LANES).astype(bf16)
            if u == 0:
                if c == 0:
                    pl.semaphore_wait(barrier, 2 * team - 1)
                both = lambda row, place, other: send_h.at[0, c, row * side + place]
                keep(both, recv_h0.at[c, me], 0, c)

                @pl.loop(1, team)
                def _(n):
                    send(both, recv_h0.at[c, me], 0, c, n, False)
            else:
                left = lambda row, place, other: send_h.at[1, c, row * side + place, 0]
                right = lambda row, place, other: send_h.at[1, c, row * side + place, 1]
                keep(left, recv_l1.at[c, my_half * team + me], 1, c)
                keep(right, recv_r1.at[c, me], 2, c)
                send(left, recv_l1.at[c, my_half * team + me], 1, c, 0, True)

                @pl.loop(1, team)
                def _(n):
                    send(left, recv_l1.at[c, my_half * team + me], 1, c, n, True)
                    send(left, recv_l1.at[c, my_half * team + me], 1, c, n, False)
                    send(right, recv_r1.at[c, me], 2, c, n, False)
        if u == 0:
            rest_of_setup()
        for t in range(0, width, step):
            gt[:, t:t + step] = jax.nn.sigmoid(
                jnp.dot(gwt[u], nt[:, t:t + step], preferred_element_type=f32)
            )
        for c in range(chunks):
            if u == 0:
                arrive(recv_h0.at[c], 0, c)
                sources = [
                    (matrix, e, 0, lambda d, s=s, e=e: recv_h0[c, d, s, e])
                    for s, matrix in enumerate((ml, mr)) for e in range(each)
                ]
            else:
                arrive(recv_l1.at[c], 1, c)
                arrive(recv_r1.at[c], 2, c)
                sources = [
                    (ml, e, h, lambda d, h=h, e=e: recv_l1[c, h * team + d, e])
                    for h in range(2) for e in range(each)
                ] + [(mr, e, 0, lambda d, e=e: recv_r1[c, d, e]) for e in range(each)]
            moved = regroup([
                [
                    get(r * side + g * fold + i)
                    for _, _, _, get in sources for r in range(rows) for g in range(groups)
                ]
                for i in range(fold)
            ])
            at = 0
            for matrix, e, h, _ in sources:
                for r in range(rows):
                    for g in range(groups):
                        lane = (h * groups + g) * LANES
                        for a in range(fold):
                            matrix[e, r * first + a * depth:r * first + (a + 1) * depth,
                                   lane:lane + LANES] = tile_of(moved, at, a)
                        at += 1
            wide_groups = 2 * groups if u == 0 else groups
            triangles = []
            for e in range(each):
                if u == 0:
                    pair = ml[e, :, :groups * LANES], mr[e]
                    over = (((1,), (1,)), ((), ()))
                else:
                    pair = ml[e], mr[e]
                    over = (((0,), (0,)), ((), ()))
                triangles.append(
                    lax.dot_general(*pair, over, preferred_element_type=f32).astype(bf16)
                )
            moved = regroup([
                [
                    tile_of(triangles[e], r * fold + a, g)
                    for e in range(each) for r in range(rows) for g in range(wide_groups)
                ]
                for a in range(fold)
            ])
            at = 0
            out = send_t0 if u == 0 else send_t1
            for e in range(each):
                for r in range(rows):
                    for g in range(wide_groups):
                        for i in range(fold):
                            place = g * fold + i
                            half, place = place // side, place % side
                            tile = tile_of(moved, at, i)
                            if u == 0:
                                out[c, half, r * side + place, e] = tile
                            else:
                                out[c, r * side + place, e] = tile
                        at += 1
            if u == 0:
                sums = lambda row, place, other: send_t0.at[
                    c, 1 - my_half if other else my_half, row * side + place
                ]
                keep(sums, recv_t0.at[c, my_half * team + me], 3, c)
                send(sums, recv_t0.at[c, my_half * team + me], 3, c, 0, True)

                @pl.loop(1, team)
                def _(n):
                    send(sums, recv_t0.at[c, my_half * team + me], 3, c, n, True)
                    send(sums, recv_t0.at[c, my_half * team + me], 3, c, n, False)
            else:
                made = lambda row, place, other: send_t1.at[c, row * side + place]
                keep(made, recv_t1.at[c, me], 4, c)

                @pl.loop(1, team)
                def _(n):
                    send(made, recv_t1.at[c, me], 4, c, n, False)
        for c in range(chunks):
            if u == 0:
                arrive(recv_t0.at[c], 3, c)
                total = recv_t0[c, :team].astype(f32) + recv_t0[c, team:].astype(f32)
            else:
                arrive(recv_t1.at[c], 4, c)
                total = recv_t1[c].astype(f32)
            back[...] = total.reshape(block * depth, LANES)
            for q in range(depth):
                tt[c * block:(c + 1) * block, q * LANES:(q + 1) * LANES] = (
                    back[pl.ds(q, block, stride=depth), :]
                )
        for t in range(0, width, step):
            mixed = norm_columns(tt[:, t:t + step], gain_out).astype(bf16)
            update = jnp.dot(owt[u], mixed, preferred_element_type=f32)
            xt[:, t:t + step] = (
                (xt[:, t:t + step] + gt[:, t:t + step] * update).astype(bf16).astype(f32)
            )
    for q in range(depth):
        tile = xt[:, q * LANES:(q + 1) * LANES].T.astype(bf16)
        for a in range(fold):
            o_ref[a * depth + q] = tile[a * second:(a + 1) * second]

    def gone(buffer, kind, slot):
        pltpu.make_async_copy(buffer, buffer, sems.at[2 * kind, slot]).wait()

    for c in range(chunks):
        gone(recv_h0.at[c, pl.ds(0, team - 1)], 0, c)
        gone(recv_l1.at[c, pl.ds(0, 2 * team - 1)], 1, c)
        gone(recv_r1.at[c, pl.ds(0, team - 1)], 2, c)
        gone(recv_t0.at[c, pl.ds(0, 2 * team - 1)], 3, c)
        gone(recv_t1.at[c, pl.ds(0, team - 1)], 4, c)


def takes(rows, cols, first, second, channels, hidden):
    if LANES % second or channels != LANES or hidden != LANES or cols % 2:
        return False
    team, fold = rows * (cols // 2), LANES // second
    return (
        CHUNK % team == 0 and first % fold == 0 and (first // fold) % PACK == 0
        and (cols // 2) % fold == 0 and first * second <= 2048
    )


def solution(mesh):
    rows, cols = mesh.shape["row"], mesh.shape["col"]

    def local(pair_rep, proj_weight, gate_weight, out_weight, in_gain, out_gain):
        first, second, channels = pair_rep.shape
        hidden = out_weight.shape[1]
        args = (pair_rep, proj_weight, gate_weight, out_weight, in_gain, out_gain)
        if not takes(rows, cols, first, second, channels, hidden):
            return plain(*args)
        team = rows * (cols // 2)
        fold = LANES // second
        depth = first // fold
        chunks = hidden // CHUNK
        each = CHUNK // team
        width = depth * LANES
        vmem = pl.BlockSpec(memory_space=pltpu.VMEM)
        return pl.pallas_call(
            functools.partial(kernel, rows, cols),
            out_shape=jax.ShapeDtypeStruct(pair_rep.shape, bf16),
            in_specs=[vmem] * 6,
            out_specs=vmem,
            scratch_shapes=[
                pltpu.VMEM((channels, width), f32),
                pltpu.VMEM((channels, width), bf16),
                pltpu.VMEM((channels, width), f32),
                pltpu.VMEM((hidden, width), f32),
                pltpu.VMEM((2, chunks, 4 * CHUNK, channels), bf16),
                pltpu.VMEM((2, channels, channels), bf16),
                pltpu.VMEM((2, channels, hidden), bf16),
                pltpu.VMEM((fold * LANES, fold * LANES), bf16),
                pltpu.VMEM((2, CHUNK * depth, LANES), f32),
                pltpu.VMEM((CHUNK * depth, LANES), f32),
                pltpu.VMEM((2, chunks, team, 2, each, depth, LANES), bf16),
                pltpu.VMEM((chunks, team, 2, each, depth, LANES), bf16),
                pltpu.VMEM((chunks, 2 * team, each, depth, LANES), bf16),
                pltpu.VMEM((chunks, team, each, depth, LANES), bf16),
                pltpu.VMEM((chunks, 2, team, each, depth, LANES), bf16),
                pltpu.VMEM((chunks, 2 * team, each, depth, LANES), bf16),
                pltpu.VMEM((chunks, team, each, depth, LANES), bf16),
                pltpu.VMEM((chunks, team, each, depth, LANES), bf16),
                pltpu.VMEM((each, rows * first, cols * second), bf16),
                pltpu.VMEM((each, rows * first, cols // 2 * second), bf16),
                pltpu.SemaphoreType.DMA((10, chunks)),
            ],
            compiler_params=pltpu.CompilerParams(collective_id=0, has_side_effects=True),
        )(*args)

    return jax.shard_map(
        local,
        mesh=mesh,
        in_specs=(P("row", "col", None), P(), P(), P(), P(), P()),
        out_specs=P("row", "col", None),
        check_vma=False,
    )
```

```python
import functools

import jax
import jax.numpy as jnp
from jax import lax
from jax.experimental import pallas as pl
from jax.experimental.pallas import tpu as pltpu
from jax.sharding import PartitionSpec as P

epsilon = 1e-05
LANES = 128
PACK = 16
CHUNK = 16
f32 = jnp.float32
bf16 = jnp.bfloat16


def layer_norm(values, gain_row, reduce_axis):
    center = values - jnp.mean(values, axis=reduce_axis, keepdims=True)
    spread = jnp.mean(center * center, axis=reduce_axis, keepdims=True)
    return center * lax.rsqrt(spread + epsilon) * gain_row


def plain(pair_rep, proj_weight, gate_weight, out_weight, in_gain, out_gain):
    current = pair_rep
    for update_index in range(2):
        widened = current.astype(f32)
        normed = layer_norm(widened, in_gain[update_index], 2).astype(bf16)
        projected = jnp.einsum(
            "ijc,pch->phij", normed, proj_weight[update_index], preferred_element_type=f32
        )
        left_hand = (jax.nn.sigmoid(projected[0]) * projected[1]).astype(bf16)
        right_hand = (jax.nn.sigmoid(projected[2]) * projected[3]).astype(bf16)
        gating = jax.nn.sigmoid(
            jnp.dot(normed, gate_weight[update_index], preferred_element_type=f32)
        )
        left_rows, right_rows = (
            lax.all_to_all(left_hand, "col", split_axis=0, concat_axis=2, tiled=True),
            lax.all_to_all(right_hand, "col", split_axis=0, concat_axis=2, tiled=True),
        )
        if update_index == 0:
            triangle = jnp.einsum(
                "gik,gjk->igj",
                left_rows,
                lax.all_gather(right_rows, "row", axis=1, tiled=True),
                preferred_element_type=f32,
            )
        else:
            left_columns = lax.all_to_all(left_rows, "row", split_axis=2, concat_axis=1, tiled=True)
            triangle = jnp.einsum(
                "gki,gkj->igj",
                left_columns,
                lax.all_gather(right_rows, "row", axis=1, tiled=True),
                preferred_element_type=f32,
            )
        returned = lax.all_to_all(
            triangle.astype(bf16), "col", split_axis=2, concat_axis=1, tiled=True
        )
        mixed_rows = layer_norm(
            returned.astype(f32), out_gain[update_index][None, :, None], 1
        ).astype(bf16)
        update = jnp.einsum(
            "ihj,hc->ijc", mixed_rows, out_weight[update_index], preferred_element_type=f32
        )
        current = (widened + gating * update).astype(bf16)
    return current


def norm_columns(values, gain_column):
    scale = 1.0 / values.shape[0]
    center = values - jnp.sum(values, axis=0, keepdims=True) * scale
    spread = jnp.sum(center * center, axis=0, keepdims=True) * scale
    return center * lax.rsqrt(spread + epsilon) * gain_column


def kernel(rows, cols, x_ref, pw_ref, gw_ref, ow_ref, ig_ref, og_ref, o_ref,
           xt, nt, gt, tt, wt, gwt, owt, perm, shuffle, back,
           send_h, recv_h0, recv_l1, recv_r1, send_t0, recv_t0, send_t1, recv_t1, ml, mr, sems):
    first, second, channels = x_ref.shape
    hidden = ow_ref.shape[1]
    side = cols // 2
    team = rows * side
    fold = LANES // second
    depth = first // fold
    block = CHUNK
    chunks = hidden // block
    each = block // team
    groups = side // fold
    width = depth * LANES
    step = min(width, 512)
    my_row, my_col = lax.axis_index("row"), lax.axis_index("col")
    my_half, my_side = my_col // side, my_col % side
    me = my_row * side + my_side

    def mate(n):
        m = (n * 13) % team if team % 13 else n
        row, place = (my_row + m % rows) % rows, (my_side + m // rows) % side
        return row, place

    def device(n, other):
        row, place = mate(n)
        return row, (1 - my_half if other else my_half) * side + place

    barrier = pltpu.get_barrier_semaphore()

    def greet(n, other):
        pl.semaphore_signal(
            barrier, inc=1, device_id=device(n, other), device_id_type=pl.DeviceIdType.MESH
        )

    greet(0, True)

    @pl.loop(1, team)
    def _(n):
        greet(n, True)
        greet(n, False)

    def send(source, target, kind, slot, n, other):
        row, place = mate(n)
        pltpu.make_async_remote_copy(
            src_ref=source(row, place, other),
            dst_ref=target,
            send_sem=sems.at[2 * kind, slot],
            recv_sem=sems.at[2 * kind + 1, slot],
            device_id=device(n, other),
            device_id_type=pl.DeviceIdType.MESH,
        ).start()

    def keep(source, target, kind, slot):
        pltpu.make_async_copy(
            source(my_row, my_side, False), target, sems.at[2 * kind + 1, slot]
        ).start()

    def arrive(buffer, kind, slot):
        pltpu.make_async_copy(buffer, buffer, sems.at[2 * kind + 1, slot]).wait()

    def weight_turn(u):
        for p in range(4):
            turned = pw_ref[u, p].astype(f32).T.astype(bf16)
            for c in range(chunks):
                wt[u, c, p * block:(p + 1) * block, :] = turned[c * block:(c + 1) * block]

    weight_turn(0)
    for q in range(depth):
        tile = jnp.concatenate([x_ref[a * depth + q] for a in range(fold)], axis=0)
        xt[:, q * LANES:(q + 1) * LANES] = tile.astype(f32).T

    def rest_of_setup():
        weight_turn(1)
        for u in range(2):
            gwt[u] = gw_ref[u].astype(f32).T.astype(bf16)
            owt[u] = ow_ref[u].astype(f32).T.astype(bf16)
        size = fold * LANES
        bits, low = LANES.bit_length() - 1, second.bit_length() - 1
        to = lax.broadcasted_iota(jnp.int32, (1, size), 1)
        at = lax.broadcasted_iota(jnp.int32, (size, size), 0)
        wanted = (
            (((to & (LANES - 1)) >> low) << bits) + ((to >> bits) << low) + (to & (second - 1))
        )
        perm[...] = jnp.where(at == wanted, 1.0, 0.0).astype(bf16)

    def regroup(parts):
        wide = jnp.concatenate([jnp.concatenate(tiles, axis=0) for tiles in parts], axis=1)
        return jnp.dot(wide, perm[...], preferred_element_type=f32).astype(bf16)

    def tile_of(array, row, lane):
        return array[row * depth:(row + 1) * depth, lane * LANES:(lane + 1) * LANES]

    for u in range(2):
        gain_in = jnp.broadcast_to(ig_ref[u:u + 1, :], (LANES, channels)).T[:, :1]
        gain_out = jnp.broadcast_to(og_ref[u:u + 1, :], (LANES, hidden)).T[:, :1]
        for t in range(0, width, step):
            nt[:, t:t + step] = norm_columns(xt[:, t:t + step], gain_in).astype(bf16)
        for c in range(chunks):
            for t in range(0, width, step):
                got = jnp.dot(wt[u, c], nt[:, t:t + step], preferred_element_type=f32)
                for s in range(2):
                    base = 2 * s * block
                    hand = jax.nn.sigmoid(got[base:base + block]) * got[base + block:base + 2 * block]
                    for k in range(step // LANES):
                        shuffle[s, pl.ds(t // LANES + k, block, stride=depth), :] = (
                            hand[:, k * LANES:(k + 1) * LANES]
                        )
            for s in range(2):
                send_h[u, c, :, s] = shuffle[s].reshape(team, each, depth, LANES).astype(bf16)
            if u == 0:
                if c == 0:
                    pl.semaphore_wait(barrier, 2 * team - 1)
                both = lambda row, place, other: send_h.at[0, c, row * side + place]
                keep(both, recv_h0.at[c, me], 0, c)

                @pl.loop(1, team)
                def _(n):
                    send(both, recv_h0.at[c, me], 0, c, n, False)
            else:
                left = lambda row, place, other: send_h.at[1, c, row * side + place, 0]
                right = lambda row, place, other: send_h.at[1, c, row * side + place, 1]
                keep(left, recv_l1.at[c, my_half * team + me], 1, c)
                keep(right, recv_r1.at[c, me], 2, c)
                send(left, recv_l1.at[c, my_half * team + me], 1, c, 0, True)

                @pl.loop(1, team)
                def _(n):
                    send(left, recv_l1.at[c, my_half * team + me], 1, c, n, True)
                    send(left, recv_l1.at[c, my_half * team + me], 1, c, n, False)
                    send(right, recv_r1.at[c, me], 2, c, n, False)
        if u == 0:
            rest_of_setup()
        for t in range(0, width, step):
            gt[:, t:t + step] = jax.nn.sigmoid(
                jnp.dot(gwt[u], nt[:, t:t + step], preferred_element_type=f32)
            )
        for c in range(chunks):
            if u == 0:
                arrive(recv_h0.at[c], 0, c)
                sources = [
                    (matrix, e, 0, lambda d, s=s, e=e: recv_h0[c, d, s, e])
                    for s, matrix in enumerate((ml, mr)) for e in range(each)
                ]
            else:
                arrive(recv_l1.at[c], 1, c)
                arrive(recv_r1.at[c], 2, c)
                sources = [
                    (ml, e, h, lambda d, h=h, e=e: recv_l1[c, h * team + d, e])
                    for h in range(2) for e in range(each)
                ] + [(mr, e, 0, lambda d, e=e: recv_r1[c, d, e]) for e in range(each)]
            moved = regroup([
                [
                    get(r * side + g * fold + i)
                    for _, _, _, get in sources for r in range(rows) for g in range(groups)
                ]
                for i in range(fold)
            ])
            at = 0
            for matrix, e, h, _ in sources:
                for r in range(rows):
                    for g in range(groups):
                        lane = (h * groups + g) * LANES
                        for a in range(fold):
                            matrix[e, r * first + a * depth:r * first + (a + 1) * depth,
                                   lane:lane + LANES] = tile_of(moved, at, a)
                        at += 1
            wide_groups = 2 * groups if u == 0 else groups
            triangles = []
            for e in range(each):
                if u == 0:
                    pair = ml[e, :, :groups * LANES], mr[e]
                    over = (((1,), (1,)), ((), ()))
                else:
                    pair = ml[e], mr[e]
                    over = (((0,), (0,)), ((), ()))
                triangles.append(
                    lax.dot_general(*pair, over, preferred_element_type=f32).astype(bf16)
                )
            moved = regroup([
                [
                    tile_of(triangles[e], r * fold + a, g)
                    for e in range(each) for r in range(rows) for g in range(wide_groups)
                ]
                for a in range(fold)
            ])
            at = 0
            out = send_t0 if u == 0 else send_t1
            for e in range(each):
                for r in range(rows):
                    for g in range(wide_groups):
                        for i in range(fold):
                            place = g * fold + i
                            half, place = place // side, place % side
                            tile = tile_of(moved, at, i)
                            if u == 0:
                                out[c, half, r * side + place, e] = tile
                            else:
                                out[c, r * side + place, e] = tile
                        at += 1
            if u == 0:
                sums = lambda row, place, other: send_t0.at[
                    c, 1 - my_half if other else my_half, row * side + place
                ]
                keep(sums, recv_t0.at[c, my_half * team + me], 3, c)
                send(sums, recv_t0.at[c, my_half * team + me], 3, c, 0, True)

                @pl.loop(1, team)
                def _(n):
                    send(sums, recv_t0.at[c, my_half * team + me], 3, c, n, True)
                    send(sums, recv_t0.at[c, my_half * team + me], 3, c, n, False)
            else:
                made = lambda row, place, other: send_t1.at[c, row * side + place]
                keep(made, recv_t1.at[c, me], 4, c)

                @pl.loop(1, team)
                def _(n):
                    send(made, recv_t1.at[c, me], 4, c, n, False)
        for c in range(chunks):
            if u == 0:
                arrive(recv_t0.at[c], 3, c)
                total = recv_t0[c, :team].astype(f32) + recv_t0[c, team:].astype(f32)
            else:
                arrive(recv_t1.at[c], 4, c)
                total = recv_t1[c].astype(f32)
            back[...] = total.reshape(block * depth, LANES)
            for q in range(depth):
                tt[c * block:(c + 1) * block, q * LANES:(q + 1) * LANES] = (
                    back[pl.ds(q, block, stride=depth), :]
                )
        for t in range(0, width, step):
            mixed = norm_columns(tt[:, t:t + step], gain_out).astype(bf16)
            update = jnp.dot(owt[u], mixed, preferred_element_type=f32)
            xt[:, t:t + step] = (
                (xt[:, t:t + step] + gt[:, t:t + step] * update).astype(bf16).astype(f32)
            )
    o_ref[...] = xt[...].astype(bf16)

    def gone(buffer, kind, slot):
        pltpu.make_async_copy(buffer, buffer, sems.at[2 * kind, slot]).wait()

    for c in range(chunks):
        gone(recv_h0.at[c, pl.ds(0, team - 1)], 0, c)
        gone(recv_l1.at[c, pl.ds(0, 2 * team - 1)], 1, c)
        gone(recv_r1.at[c, pl.ds(0, team - 1)], 2, c)
        gone(recv_t0.at[c, pl.ds(0, 2 * team - 1)], 3, c)
        gone(recv_t1.at[c, pl.ds(0, team - 1)], 4, c)


def finish(fold, t_ref, o_ref):
    first, second, _ = o_ref.shape
    depth = first // fold
    for q in range(depth):
        tile = t_ref[:, q * LANES:(q + 1) * LANES].astype(f32).T.astype(bf16)
        for a in range(fold):
            o_ref[a * depth + q] = tile[a * second:(a + 1) * second]


def takes(rows, cols, first, second, channels, hidden):
    if LANES % second or channels != LANES or hidden != LANES or cols % 2:
        return False
    team, fold = rows * (cols // 2), LANES // second
    return (
        CHUNK % team == 0 and first % fold == 0 and (first // fold) % PACK == 0
        and (cols // 2) % fold == 0 and first * second <= 2048
    )


def solution(mesh):
    rows, cols = mesh.shape["row"], mesh.shape["col"]

    def local(pair_rep, proj_weight, gate_weight, out_weight, in_gain, out_gain):
        first, second, channels = pair_rep.shape
        hidden = out_weight.shape[1]
        args = (pair_rep, proj_weight, gate_weight, out_weight, in_gain, out_gain)
        if not takes(rows, cols, first, second, channels, hidden):
            return plain(*args)
        team = rows * (cols // 2)
        fold = LANES // second
        depth = first // fold
        chunks = hidden // CHUNK
        each = CHUNK // team
        width = depth * LANES
        vmem = pl.BlockSpec(memory_space=pltpu.VMEM)
        turned = pl.pallas_call(
            functools.partial(kernel, rows, cols),
            out_shape=jax.ShapeDtypeStruct((channels, width), bf16),
            in_specs=[vmem] * 6,
            out_specs=vmem,
            scratch_shapes=[
                pltpu.VMEM((channels, width), f32),
                pltpu.VMEM((channels, width), bf16),
                pltpu.VMEM((channels, width), f32),
                pltpu.VMEM((hidden, width), f32),
                pltpu.VMEM((2, chunks, 4 * CHUNK, channels), bf16),
                pltpu.VMEM((2, channels, channels), bf16),
                pltpu.VMEM((2, channels, hidden), bf16),
                pltpu.VMEM((fold * LANES, fold * LANES), bf16),
                pltpu.VMEM((2, CHUNK * depth, LANES), f32),
                pltpu.VMEM((CHUNK * depth, LANES), f32),
                pltpu.VMEM((2, chunks, team, 2, each, depth, LANES), bf16),
                pltpu.VMEM((chunks, team, 2, each, depth, LANES), bf16),
                pltpu.VMEM((chunks, 2 * team, each, depth, LANES), bf16),
                pltpu.VMEM((chunks, team, each, depth, LANES), bf16),
                pltpu.VMEM((chunks, 2, team, each, depth, LANES), bf16),
                pltpu.VMEM((chunks, 2 * team, each, depth, LANES), bf16),
                pltpu.VMEM((chunks, team, each, depth, LANES), bf16),
                pltpu.VMEM((chunks, team, each, depth, LANES), bf16),
                pltpu.VMEM((each, rows * first, cols * second), bf16),
                pltpu.VMEM((each, rows * first, cols // 2 * second), bf16),
                pltpu.SemaphoreType.DMA((10, chunks)),
            ],
            compiler_params=pltpu.CompilerParams(collective_id=0, has_side_effects=True),
        )(*args)
        return pl.pallas_call(
            functools.partial(finish, fold),
            out_shape=jax.ShapeDtypeStruct(pair_rep.shape, bf16),
            in_specs=[vmem],
            out_specs=vmem,
        )(turned)

    return jax.shard_map(
        local,
        mesh=mesh,
        in_specs=(P("row", "col", None), P(), P(), P(), P(), P()),
        out_specs=P("row", "col", None),
        check_vma=False,
    )
```
